32 devices in a mesh: section: 16 (over z, x, core), tp: 2 (over y).
Axes of the slice: x: 2, y: 2, z: 4, core: 2. Of those that a mesh axis runs over, the one named last changes fastest.
Arguments:
- carried: bfloat16 [16, 256, 5120], P('section', 'tp'), may hold values from -6 to 6
- carried_segments: int32 [16, 256], P('section'), may hold values from 0 to 31, as said below
- fresh_batch: bfloat16 [2, 256, 5120], P(None, 'tp'), may hold values from -6 to 6
- fresh_segments: int32 [2, 256], replicated, may hold values from 0 to 31, as said below
- qkv_weight: bfloat16 [16, 5120, 3, 2048], P('section', None, None, 'tp'), may hold values from -3.354102 to 3.354102
- out_weight: bfloat16 [16, 2048, 5120], P('section', 'tp'), may hold values from -0.09375 to 0.09375
- norm_gain: bfloat16 [16, 2560], P('section'), may hold values from 0.099609375 to 1.8984375
Outputs:
- layer_outputs: bfloat16 [2, 16, 256, 5120], P(None, 'section', 'tp')
- shadow_outputs: bfloat16 [16, 256, 5120], P('section', 'tp')
The draws below stay inside these ranges and needn't reach their ends.
Inputs may be any that keep to these rules, and one draw needn't show every extreme that they name: `carried_segments`: document ids of each micro-batch's 512 tokens, read in token order across its two halves, start at 0, never fall, and rise by one at each document start; every micro-batch holds exactly 32 documents. `fresh_segments`: the same law for the entering micro-batch.
All inputs are finite; a program needn't handle non-finite values.
Results may differ from the reference program's by a relative error of at most 0.019.
Values may be sent and summed in bfloat16 or wider, within the bound.
A program may use at most 128 MiB of HBM per device.

```python
import jax
import jax.numpy as jnp
from jax import lax

D = 5120
HEADS = 32
HD = 128
TOK = 512
STEPS = 2
SECTIONS = 8
HALF = 256
N_TP = 2


def segment_ids(key, count):
    pieces = max(2, TOK // 16)
    keys = jax.random.split(key, count)
    orders = jax.vmap(lambda single: jax.random.permutation(single, TOK - 1))(keys)
    chosen = orders[:, :pieces - 1] + 1
    marks = jnp.zeros((count, TOK), jnp.int32)
    marks = marks.at[jnp.arange(count)[:, None], chosen].set(1)
    marks = marks.at[:, 0].set(1)
    return (jnp.cumsum(marks, axis=1) - 1).astype(jnp.int32)


def draw_carried_segments(key, part):
    return segment_ids(jax.random.fold_in(key, 21), SECTIONS).reshape(SECTIONS * 2, TOK // 2)


def draw_fresh_segments(key, part):
    return segment_ids(jax.random.fold_in(key, 22), 1).reshape(2, TOK // 2)


def draw_qkv_weight(key, part):
    columns = HEADS * HD // 2
    drawn = jax.random.truncated_normal(jax.random.fold_in(key, 11), -6.0, 6.0, (SECTIONS * 2, D, 3, columns), jnp.float32) * D ** (-0.5)
    return drawn.astype(jnp.bfloat16)


def levels(own_key, extent, cuts, smallest, high):
    loudness = 1.0
    for position, blocks in cuts:
        steps = jax.random.uniform(jax.random.fold_in(jax.random.fold_in(own_key, 6), position), (blocks,), jnp.float32, smallest / len(cuts), high / len(cuts))
        loudness = loudness * jnp.repeat(jnp.exp(steps), extent[position] // blocks).reshape((-1,) + (1,) * (len(extent) - 1 - position))
    return loudness


def normal_values(own_key, dims, spread, reach, cuts=(), held_as=jnp.bfloat16):
    level = levels(own_key, dims, cuts, -0.22, 0.18) if cuts else 1.0
    values = jax.random.normal(own_key, dims, jnp.float32) * spread * level
    return jnp.minimum(jnp.maximum(values, -reach), reach).astype(held_as)


def setup_inputs(seed: int = 0) -> dict:
    arg_keys = jax.random.split(jax.random.key(seed), 8)
    carried = normal_values(arg_keys[0], (2 * SECTIONS, HALF, D), 1.0, 6.0, ((0, 16), (1, 2)))
    carried_segments = draw_carried_segments(jax.random.fold_in(arg_keys[7], 71), 0)
    fresh_batch = normal_values(arg_keys[2], (2, HALF, D), 1.0, 6.0, ((1, 2),))
    fresh_segments = draw_fresh_segments(jax.random.fold_in(arg_keys[7], 71), 0)
    qkv_weight = draw_qkv_weight(jax.random.fold_in(arg_keys[7], 71), 0)
    out_weight = normal_values(arg_keys[5], (2 * SECTIONS, HEADS * HD // 2, D), (HEADS * HD) ** -0.5, 0.09375, ((0, 16), (1, 2)))
    norm_gain = jnp.clip(1.0 + 0.18 * jax.random.normal(arg_keys[6], (2 * SECTIONS, D // 2), jnp.float32), 0.099609375, 1.8984375).astype(jnp.bfloat16)
    return dict(carried=carried, carried_segments=carried_segments, fresh_batch=fresh_batch, fresh_segments=fresh_segments, qkv_weight=qkv_weight, out_weight=out_weight, norm_gain=norm_gain)


eps = 1e-05
rope_base = 10000.0

def normalize(values, gain):
    widened = values.astype(jnp.float32)
    power = lax.optimization_barrier(jnp.mean(widened * widened, axis=-1, keepdims=True))
    return (widened * lax.rsqrt(power + eps) * gain.astype(jnp.float32)).astype(jnp.bfloat16)

def rotate(values, positions):
    half_dim = values.shape[-1] // 2
    frequency = rope_base ** (-(jnp.arange(half_dim, dtype=jnp.float32) * 2.0 / values.shape[-1]))
    angles = positions.astype(jnp.float32)[:, None] * frequency[None, :]
    cosine = jnp.cos(angles)[:, None, :]
    sine = jnp.sin(angles)[:, None, :]
    leading = values[..., :half_dim]
    trailing = values[..., half_dim:]
    return jnp.concatenate([leading * cosine - trailing * sine, trailing * cosine + leading * sine], axis=-1)

def attend(projected, positions, segments):
    count = projected.shape[0]
    width = projected.shape[1] // 3
    parts = projected.reshape(count, 3, width // HD, HD)
    queries = rotate(parts[:, 0], positions).astype(jnp.bfloat16)
    keyed = rotate(parts[:, 1], positions).astype(jnp.bfloat16)
    values = parts[:, 2].astype(jnp.bfloat16)
    scores = jnp.einsum('qhd,khd->hqk', queries.astype(jnp.float32), keyed.astype(jnp.float32)) * HD ** (-0.5)
    visible = (positions[None, :] <= positions[:, None]) & (segments[None, :] == segments[:, None])
    masked = jnp.where(visible[None], scores, -1e+30)
    highest = lax.optimization_barrier(jnp.max(masked, axis=-1, keepdims=True))
    weights = jnp.where(visible[None], jnp.exp(masked - highest), 0.0)
    shares = (weights / lax.optimization_barrier(jnp.sum(weights, axis=-1, keepdims=True))).astype(jnp.bfloat16)
    mixed = jnp.einsum('hqk,khd->qhd', shares.astype(jnp.float32), values.astype(jnp.float32))
    return mixed.astype(jnp.bfloat16).reshape(count, width)

def layer(bundle):
    rows, segments, gain, weights_in, weights_out = bundle
    matrix = jnp.transpose(weights_in, (1, 2, 0, 3)).reshape(D, 3 * HEADS * HD)
    normed = normalize(rows, gain)
    projected = jnp.dot(normed, matrix, preferred_element_type=jnp.float32)
    positions = jnp.arange(TOK, dtype=jnp.int32)
    mixed = attend(projected, positions, segments)
    groups = 2 * N_TP
    width = HEADS * HD // groups
    blocks = mixed.reshape(TOK, groups, width).astype(jnp.float32)
    out_blocks = weights_out.reshape(groups, width, D).astype(jnp.float32)
    partials = jnp.einsum('tgc,gcd->gtd', blocks, out_blocks)
    rounded = lax.optimization_barrier(partials.astype(jnp.bfloat16)).astype(jnp.float32)
    return (rows.astype(jnp.float32) + lax.optimization_barrier(jnp.sum(rounded, axis=0))).astype(jnp.bfloat16)

def reference(carried, carried_segments, fresh_batch, fresh_segments, qkv_weight, out_weight, norm_gain):
    inputs_one = carried.reshape(SECTIONS, TOK, D)
    segments_one = carried_segments.reshape(SECTIONS, TOK)
    gains = norm_gain.reshape(SECTIONS, D)
    weights_in = qkv_weight.reshape(SECTIONS, 2, D, 3, HEADS * HD // 2)
    weights_out = out_weight.reshape(SECTIONS, HEADS * HD, D)
    outputs_one = lax.map(layer, (inputs_one, segments_one, gains, weights_in, weights_out))
    inputs_two = jnp.concatenate([fresh_batch.reshape(1, TOK, D), outputs_one[:-1]], axis=0)
    segments_two = jnp.concatenate([fresh_segments.reshape(1, TOK), segments_one[:-1]], axis=0)
    outputs_two = lax.map(layer, (inputs_two, segments_two, gains, weights_in, weights_out))
    shadow = jnp.concatenate([outputs_two[1:], jnp.zeros((1, TOK, D), jnp.bfloat16)], axis=0)
    stacked = jnp.stack([outputs_one, outputs_two]).reshape(STEPS, 2 * SECTIONS, HALF, D)
    return (stacked, shadow.reshape(2 * SECTIONS, HALF, D))
```

```python
import functools

import jax
import jax.numpy as jnp
import numpy as np
from jax import lax
from jax.experimental import pallas as pl
from jax.experimental.pallas import tpu as pltpu
from jax.sharding import PartitionSpec as P

HD = 128
LANES = 128
LOG2E = 1.4426950408889634
TILE = 512
CHUNK = 1024
PARTS = 2
NORM_ROWS = 16
SEND_AT = 5
RELAY_AT = 3
MESH = pl.DeviceIdType.MESH

eps = 1e-05
rope_base = 10000.0


def relay_kernel(
    groups,
    sections,
    x_hbm,
    segments_hbm,
    fresh_hbm,
    fresh_segments_hbm,
    weights_in_hbm,
    weights_out_hbm,
    gain_hbm,
    cosine_hbm,
    sine_hbm,
    out_hbm,
    shadow_hbm,
    weights_in,
    weights_out,
    gathered,
    qkv,
    mixed,
    kept,
    give_out,
    give_in,
    arrived,
    rows_in,
    staged,
    cosine,
    sine,
    bias,
    pieces,
    ids,
    gain_raw,
    gain_pieces,
    gain,
    load_sem,
    tile_sem,
    chunk_sem,
    own_row_sem,
    next_row_sem,
    small_send,
    small_recv,
    own_send,
    own_recv,
    share_send,
    share_recv,
    relay_send,
    relay_recv,
    give_send,
    give_recv,
    sum_send,
    sum_recv,
    shift_send,
    shift_recv,
    back_send,
    back_recv,
    store_sem,
    free_sem,
):
    place = lax.axis_index("section")
    mine = lax.axis_index("tp")
    parity = place % 2
    core = (place + 1 - 2 * parity, mine)
    has_next, has_previous = place + 2 < sections, place >= 2
    ahead, behind = (place + 2, mine), (place - 2, mine)

    block, depth = x_hbm.shape
    half = block * groups
    tiles, _, tile = weights_in.shape
    per_kind = tiles // 3
    chunks, width, chunk = weights_out.shape
    heads = width // HD
    part = block // PARTS

    def peer(by):
        return (mine + by) % groups

    def source(by):
        return (mine + groups - by) % groups

    def block_at(index):
        return pl.ds(pl.multiple_of(index * block, block), block)

    def remote(src, dst, send, recv, device):
        return pltpu.make_async_remote_copy(
            src_ref=src, dst_ref=dst, send_sem=send, recv_sem=recv, device_id=device, device_id_type=MESH
        )

    def tile_copy(j):
        kind = j // per_kind
        columns = pl.ds(pl.multiple_of((j % per_kind) * tile, tile), tile)
        return pltpu.make_async_copy(weights_in_hbm.at[kind, :, columns], weights_in.at[j], tile_sem.at[j])

    def columns_of(c):
        return pl.ds(pl.multiple_of(c * chunk, chunk), chunk)

    def chunk_copy(c):
        return pltpu.make_async_copy(weights_out_hbm.at[:, columns_of(c)], weights_out.at[c], chunk_sem.at[c])

    def own_rows_copy(c):
        return pltpu.make_async_copy(x_hbm.at[:, columns_of(c)], rows_in.at[0, c], own_row_sem.at[c])

    def fresh_copy(c):
        return pltpu.make_async_copy(
            fresh_hbm.at[parity, :, columns_of(c)], rows_in.at[1, c], next_row_sem.at[c]
        )

    gain_copy = pltpu.make_async_copy(gain_hbm, gain_raw, load_sem.at[0])
    ids_copy = pltpu.make_async_copy(segments_hbm, pieces.at[parity], load_sem.at[1])
    cosine_copy = pltpu.make_async_copy(cosine_hbm, cosine, load_sem.at[2])
    sine_copy = pltpu.make_async_copy(sine_hbm, sine, load_sem.at[3])
    fresh_ids_copy = pltpu.make_async_copy(fresh_segments_hbm, ids.at[1], load_sem.at[4])

    gain_send = remote(gain_pieces.at[parity], gain_pieces.at[parity], small_send.at[0], small_recv.at[0], core)
    ids_send = remote(pieces.at[parity], pieces.at[parity], small_send.at[1], small_recv.at[1], core)
    ids_ahead = remote(ids.at[0], ids.at[1], small_send.at[2], small_recv.at[2], ahead)

    gain_copy.start()
    ids_copy.start()
    for c in range(chunks):
        own_rows_copy(c).start()
    for j in range(tiles):
        tile_copy(j).start()
    cosine_copy.start()
    sine_copy.start()
    for c in range(chunks):
        chunk_copy(c).start()

    @pl.when(jnp.logical_not(has_previous))
    def _():
        fresh_ids_copy.start()
        for c in range(chunks):
            fresh_copy(c).start()

    barrier = pltpu.get_barrier_semaphore()
    pl.semaphore_signal(barrier, inc=1, device_id=core, device_id_type=MESH)
    for g in range(1, groups):
        pl.semaphore_signal(barrier, inc=1, device_id=(place, peer(g)), device_id_type=MESH)

    @pl.when(has_next)
    def _():
        pl.semaphore_signal(barrier, inc=1, device_id=ahead, device_id_type=MESH)

    @pl.when(has_previous)
    def _():
        pl.semaphore_signal(barrier, inc=1, device_id=behind, device_id_type=MESH)

    pl.semaphore_wait(barrier, groups + has_next.astype(jnp.int32) + has_previous.astype(jnp.int32))

    gain_copy.wait()
    gain_pieces[parity] = gain_raw[...].astype(jnp.float32)
    gain_send.start()
    ids_copy.wait()
    ids_send.start()

    def normalize(step):
        def some(r, carry):
            rows = pl.ds(pl.multiple_of(r * NORM_ROWS, NORM_ROWS), NORM_ROWS)
            power = jnp.zeros((NORM_ROWS, 1), jnp.float32)
            for c in range(chunks):
                widened = rows_in[step, c, rows, :].astype(jnp.float32)
                power = power + jnp.sum(widened * widened, axis=-1, keepdims=True)
            scale = lax.rsqrt(power / depth + eps)
            target = pl.ds(pl.multiple_of(parity * block + r * NORM_ROWS, NORM_ROWS), NORM_ROWS)
            for c in range(chunks):
                columns = slice(c * chunk, (c + 1) * chunk)
                widened = rows_in[step, c, rows, :].astype(jnp.float32)
                gathered[mine, target, columns] = (widened * scale * gain[:, columns]).astype(jnp.bfloat16)
            return carry

        lax.fori_loop(0, block // NORM_ROWS, some, 0)

    def own_copy():
        rows = gathered.at[mine, pl.ds(pl.multiple_of(parity * block, block), block)]
        return remote(rows, rows, own_send.at[0], own_recv.at[0], core)

    def share_copy(g, s):
        rows = gathered.at[mine, pl.ds(pl.multiple_of(parity * block + s * part, part), part)]
        slot = (g - 1) * PARTS + s
        return remote(rows, rows, share_send.at[slot], share_recv.at[slot], (place, peer(g)))

    def relay_copy(g, s, h):
        rows = gathered.at[source(g), pl.ds(h * block + s * part, part)]
        slot = (g - 1) * PARTS + s
        return remote(rows, rows, relay_send.at[slot], relay_recv.at[slot], core)

    def share():
        for s in range(PARTS):
            for g in range(1, groups):
                share_copy(g, s).start()

    def relay(s, h):
        for g in range(1, groups):
            share_copy(g, s).wait_recv()
            relay_copy(g, s, h).start()

    def project(rows, places, first, events):
        def one(j, carry):
            for at, event in events:
                pl.when(j == at)(event)
            if first:
                tile_copy(j).wait()
            kind = j // per_kind
            turning = (kind < 2).astype(jnp.float32)
            factor = turning * jnp.where(kind == 0, HD ** (-0.5) * LOG2E, 1.0)
            product = jnp.dot(rows(), weights_in[j], preferred_element_type=jnp.float32)
            column = (j % per_kind) * tile
            for i, token in enumerate(places):
                at = pl.ds(pl.multiple_of(token, block), block)
                cosines = cosine[at, :] * factor + (1.0 - turning)
                sines = sine[at, :] * factor
                for n in range(tile // HD):
                    each = product[i * block : (i + 1) * block, n * HD : (n + 1) * HD]
                    turned = each * cosines + pltpu.roll(each, HD // 2, 1) * sines
                    to = pl.ds(pl.multiple_of(column + n * HD, HD), HD)
                    qkv[kind, at, to] = turned.astype(jnp.bfloat16)
            return carry

        lax.fori_loop(0, tiles, one, 0)

    def project_others(h):
        def one(g, carry):
            index = source(g)
            project(
                lambda: gathered[index, h * block : (h + 1) * block, :],
                [h * half + index * block],
                False,
                [],
            )
            return carry

        lax.fori_loop(1, groups, one, 0)

    def find_bias(step):
        across = half // LANES
        for h in range(2):
            row = jnp.broadcast_to(ids[step, h : h + 1, :].astype(jnp.float32), (LANES, half))
            column = row.T
            for q in range(across):
                wanted = column[q * LANES : (q + 1) * LANES]
                first = h * half + q * LANES
                for k in range(h * across + q + 1):
                    given = ids[step, k // across : k // across + 1, (k % across) * LANES : (k % across + 1) * LANES]
                    seen = wanted == given.astype(jnp.float32)
                    if k == h * across + q:
                        down = lax.broadcasted_iota(jnp.int32, (LANES, LANES), 0)
                        seen = seen & (lax.broadcasted_iota(jnp.int32, (LANES, LANES), 1) <= down)
                    bias[first : first + LANES, k * LANES : (k + 1) * LANES] = jnp.where(seen, 0.0, -1e30)

    def attend(h):
        def one(n, carry):
            to = pl.ds(pl.multiple_of(n * HD, HD), HD)
            for q in range(half // LANES):
                first = h * half + q * LANES
                last = first + LANES
                scores = lax.dot_general(
                    qkv[0, first:last, to],
                    qkv[1, 0:last, to],
                    (((1,), (1,)), ((), ())),
                    preferred_element_type=jnp.float32,
                ) + bias[first:last, 0:last]
                weights = jnp.exp2(scores - jnp.max(scores, axis=-1, keepdims=True))
                total = jnp.sum(weights, axis=-1, keepdims=True)
                product = jnp.dot(
                    weights.astype(jnp.bfloat16), qkv[2, 0:last, to], preferred_element_type=jnp.float32
                )
                mixed[q * LANES : (q + 1) * LANES, to] = (product / total).astype(jnp.bfloat16)
            return carry

        lax.fori_loop(0, heads, one, 0, unroll=2)

    def give_copy(i):
        g, c = (i // chunks + 1) % groups, i % chunks
        slot = i % 2
        return remote(
            give_out.at[slot], give_in.at[c, block_at(peer(g))], give_send.at[slot], give_recv.at[i], core
        )

    def out_product(i):
        g, c = (i // chunks + 1) % groups, i % chunks
        return jnp.dot(mixed[block_at(peer(g)), :], weights_out[c], preferred_element_type=jnp.float32)

    messages = groups * chunks

    def give():
        def one(i, carry):
            @pl.when(i >= 2)
            def _():
                give_copy(i).wait_send()

            give_out[i % 2] = out_product(i).astype(jnp.bfloat16)
            give_copy(i).start()
            return carry

        lax.fori_loop(0, messages, one, 0)
        give_copy(messages - 2).wait_send()
        give_copy(messages - 1).wait_send()

    def sum_copy(i):
        g, c = i // chunks + 1, i % chunks
        return remote(
            give_in.at[c, block_at(peer(g))], arrived.at[c, g - 1], sum_send.at[i], sum_recv.at[i], (place, peer(g))
        )

    def keep_others():
        def one(i, carry):
            g, c = i // chunks + 1, i % chunks
            give_copy(i).wait_recv()
            total = out_product(i) + give_in[c, block_at(peer(g)), :].astype(jnp.float32)
            give_in[c, block_at(peer(g)), :] = total.astype(jnp.bfloat16)
            sum_copy(i).start()
            return carry

        lax.fori_loop(0, messages - chunks, one, 0)

    def keep_own(step):
        def one(i, carry):
            c = i % chunks
            give_copy(i).wait_recv()
            total = out_product(i) + give_in[c, block_at(mine), :].astype(jnp.float32)
            kept[c] = total + rows_in[step, c].astype(jnp.float32)
            return carry

        lax.fori_loop(messages - chunks, messages, one, 0)

    def store_copy(step, c):
        return pltpu.make_async_copy(staged.at[c], out_hbm.at[step, 0, :, columns_of(c)], store_sem.at[c])

    def shift_copy(c):
        return remote(staged.at[c], rows_in.at[1, c], shift_send.at[c], shift_recv.at[c], ahead)

    def back_copy(c):
        return remote(
            staged.at[c], shadow_hbm.at[0, :, columns_of(c)], back_send.at[c], back_recv.at[c], behind
        )

    def finish(step, low, high):
        def one(c, carry):
            total = kept[c]
            for g in range(1, groups):
                sum_copy((g - 1) * chunks + c).wait_recv()
                total = total + arrived[c, g - 1].astype(jnp.float32)
            staged[c] = total.astype(jnp.bfloat16)
            if step == 0:
                pl.when(has_next)(lambda: shift_copy(c).start())
            else:
                pl.when(has_previous)(lambda: back_copy(c).start())
            store_copy(step, c).start()
            return carry

        lax.fori_loop(low, high, one, 0)

    def zero_copy(c):
        return pltpu.make_async_copy(staged.at[0], shadow_hbm.at[0, :, columns_of(c)], back_recv.at[c])

    def wait_sent(copies):
        for copy in copies:
            copy.wait_send()

    every_share = [(g, s) for g in range(1, groups) for s in range(PARTS)]
    is_low, is_high = parity == 0, parity == 1

    ids_send.wait_recv()
    ids[0, 0:1, :] = pieces[0]
    ids[0, 1:2, :] = pieces[1]
    pl.when(has_next)(ids_ahead.start)
    gain_send.wait_recv()
    gain[:, 0 : depth // 2] = gain_pieces[0]
    gain[:, depth // 2 :] = gain_pieces[1]
    for c in range(chunks):
        own_rows_copy(c).wait()
    normalize(0)
    own_copy().start()
    pl.when(is_low)(share)

    @pl.when(jnp.logical_not(has_next))
    def _():
        staged[0] = jnp.zeros_like(staged[0])
        for c in range(chunks):
            zero_copy(c).start()

    cosine_copy.wait()
    sine_copy.wait()
    find_bias(0)

    for step in range(2):
        own_copy().wait_recv()

        def send_high():
            pl.when(is_high)(share)

        def relay_low():
            pl.when(is_low)(lambda: relay(0, 0))

        project(
            lambda: gathered[mine],
            [mine * block, half + mine * block],
            step == 0,
            [(min(RELAY_AT, tiles - 1), relay_low), (min(SEND_AT, tiles - 1), send_high)],
        )

        if step == 0:

            @pl.when(jnp.logical_not(has_next))
            def _():
                for c in range(chunks):
                    zero_copy(c).wait()

            for c in range(chunks):
                chunk_copy(c).wait()

        @pl.when(is_low)
        def _():
            for s in range(1, PARTS):
                relay(s, 0)

        @pl.when(is_high)
        def _():
            for g, s in every_share:
                relay_copy(g, s, 0).wait_recv()

        project_others(0)
        attend(0)

        @pl.when(is_low)
        def _():
            wait_sent([relay_copy(g, s, 0) for g, s in every_share])
            keep_others()
            keep_own(step)

        @pl.when(is_high)
        def _():
            give()
            for s in range(PARTS):
                relay(s, 1)

        @pl.when(is_low)
        def _():
            for g, s in every_share:
                relay_copy(g, s, 1).wait_recv()

        project_others(1)

        @pl.when(is_low)
        def _():
            finish(step, 0, 2)

        attend(1)

        @pl.when(is_low)
        def _():
            give()
            finish(step, 2, chunks)

        @pl.when(is_high)
        def _():
            wait_sent([relay_copy(g, s, 1) for g, s in every_share])
            keep_others()
            keep_own(step)
            finish(step, 0, chunks)

        wait_sent([sum_copy(i) for i in range(messages - chunks)])
        if step == 0:

            @pl.when(is_high)
            def _():
                pl.semaphore_signal(free_sem, inc=1, device_id=core, device_id_type=MESH)

        own_copy().wait_send()
        wait_sent([share_copy(g, s) for g, s in every_share])
        for c in range(chunks):
            store_copy(step, c).wait()
        if step == 0:

            @pl.when(has_next)
            def _():
                ids_ahead.wait_send()
                wait_sent([shift_copy(c) for c in range(chunks)])

            @pl.when(has_previous)
            def _():
                ids_ahead.wait_recv()
                for c in range(chunks):
                    shift_copy(c).wait_recv()

            @pl.when(jnp.logical_not(has_previous))
            def _():
                fresh_ids_copy.wait()
                for c in range(chunks):
                    fresh_copy(c).wait()

            normalize(1)
            own_copy().start()

            @pl.when(is_low)
            def _():
                pl.semaphore_wait(free_sem, 1)
                share()

            find_bias(1)

    gain_send.wait_send()
    ids_send.wait_send()

    @pl.when(has_previous)
    def _():
        wait_sent([back_copy(c) for c in range(chunks)])

    @pl.when(has_next)
    def _():
        for c in range(chunks):
            back_copy(c).wait_recv()


def turning(tokens):
    dim = HD // 2
    frequency = np.float32(rope_base) ** (-(np.arange(dim, dtype=np.float32) * np.float32(2.0 / HD)))
    angles = np.arange(tokens, dtype=np.float32)[:, None] * frequency.astype(np.float32)[None, :]
    cosine, sine = np.cos(angles), np.sin(angles)
    return (
        np.concatenate([cosine, cosine], -1).astype(np.float32),
        np.concatenate([-sine, sine], -1).astype(np.float32),
    )


def per_device(
    groups, sections, carried, carried_segments, fresh_batch, fresh_segments, qkv_weight, out_weight, norm_gain
):
    block, depth = carried.shape[1:]
    half = block * groups
    width = out_weight.shape[1]
    tile = min(TILE, width)
    tiles = 3 * width // tile
    chunks = depth // CHUNK
    cosine, sine = turning(2 * half)
    weights_in = jnp.transpose(qkv_weight[0], (1, 0, 2))
    near, f32 = jnp.bfloat16, jnp.float32
    dma = pltpu.SemaphoreType.DMA
    shares = (groups - 1) * PARTS
    messages = groups * chunks
    flops = 2 * (2 * 2 * half * depth * 4 * width + 4 * width * 4 * half * half)
    out, shadow = pl.pallas_call(
        functools.partial(relay_kernel, groups, sections),
        out_shape=(
            jax.ShapeDtypeStruct((2, 1, block, depth), near),
            jax.ShapeDtypeStruct((1, block, depth), near),
        ),
        in_specs=[pl.BlockSpec(memory_space=pl.ANY)] * 9,
        out_specs=(pl.BlockSpec(memory_space=pl.ANY),) * 2,
        scratch_shapes=[
            pltpu.VMEM((tiles, depth, tile), near),
            pltpu.VMEM((chunks, width, CHUNK), near),
            pltpu.VMEM((groups, 2 * block, depth), near),
            pltpu.VMEM((3, 2 * half, width), near),
            pltpu.VMEM((half, width), near),
            pltpu.VMEM((chunks, block, CHUNK), f32),
            pltpu.VMEM((2, block, CHUNK), near),
            pltpu.VMEM((chunks, half, CHUNK), near),
            pltpu.VMEM((chunks, groups - 1, block, CHUNK), near),
            pltpu.VMEM((2, chunks, block, CHUNK), near),
            pltpu.VMEM((chunks, block, CHUNK), near),
            pltpu.VMEM((2 * half, HD), f32),
            pltpu.VMEM((2 * half, HD), f32),
            pltpu.VMEM((2 * half, 2 * half), f32),
            pltpu.VMEM((2, 1, half), jnp.int32),
            pltpu.VMEM((2, 2, half), jnp.int32),
            pltpu.VMEM((1, depth // 2), near),
            pltpu.VMEM((2, 1, depth // 2), f32),
            pltpu.VMEM((1, depth), f32),
            dma((5,)),
            dma((tiles,)),
            dma((chunks,)),
            dma((chunks,)),
            dma((chunks,)),
            dma((3,)),
            dma((3,)),
            dma((1,)),
            dma((1,)),
            dma((shares,)),
            dma((shares,)),
            dma((shares,)),
            dma((shares,)),
            dma((2,)),
            dma((messages,)),
            dma((messages - chunks,)),
            dma((messages - chunks,)),
            dma((chunks,)),
            dma((chunks,)),
            dma((chunks,)),
            dma((chunks,)),
            dma((chunks,)),
            pltpu.SemaphoreType.REGULAR,
        ],
        compiler_params=pltpu.CompilerParams(
            collective_id=0, has_side_effects=True, vmem_limit_bytes=67043328
        ),
        cost_estimate=pl.CostEstimate(
            flops=flops, bytes_accessed=8 * depth * width, transcendentals=0
        ),
        name="relay",
    )(
        carried[0],
        carried_segments,
        fresh_batch,
        fresh_segments,
        weights_in,
        out_weight[0],
        norm_gain,
        cosine,
        sine,
    )
    return out, shadow


def solution(mesh):
    return jax.shard_map(
        functools.partial(per_device, mesh.shape["tp"], mesh.shape["section"]),
        mesh=mesh,
        in_specs=(
            P("section", "tp", None),
            P("section", None),
            P(None, "tp", None),
            P(),
            P("section", None, None, "tp"),
            P("section", "tp", None),
            P("section", None),
        ),
        out_specs=(P(None, "section", "tp", None), P("section", "tp", None)),
        check_vma=False,
    )
```

```python
import functools

import jax
import jax.numpy as jnp
import numpy as np
from jax import lax
from jax.experimental import pallas as pl
from jax.experimental.pallas import tpu as pltpu
from jax.sharding import PartitionSpec as P

HD = 128
LANES = 128
LOG2E = 1.4426950408889634
TILE = 512
CHUNK = 1024
PARTS = 4
NORM_ROWS = 16
PIECE = 256
RELAYS_AT = ((3, 5), (0, 0, 3))
COMBINES_AT = (1, 2, 3)
FREE_AT = 3
SHARE_AT = 4
FINISH_AT = 4
MESH = pl.DeviceIdType.MESH

eps = 1e-05
rope_base = 10000.0


def relay_kernel(
    groups,
    sections,
    x_hbm,
    segments_hbm,
    fresh_hbm,
    fresh_segments_hbm,
    weights_in_hbm,
    weights_out_hbm,
    gain_hbm,
    cosine_hbm,
    sine_hbm,
    out_hbm,
    shadow_hbm,
    weights_in,
    weights_out,
    gathered,
    qkv,
    mixed,
    partial,
    give_in,
    arrived,
    rows_in,
    staged,
    cosine,
    sine,
    bias,
    pieces,
    ids,
    gain_raw,
    gain_pieces,
    gain,
    load_sem,
    tile_sem,
    chunk_sem,
    own_row_sem,
    next_row_sem,
    small_send,
    small_recv,
    own_send,
    own_recv,
    share_send,
    share_recv,
    relay_send,
    relay_recv,
    give_send,
    give_recv,
    sum_send,
    sum_recv,
    shift_send,
    shift_recv,
    back_send,
    back_recv,
    store_sem,
    free_sem,
):
    place = lax.axis_index("section")
    mine = lax.axis_index("tp")
    parity = place % 2
    core = (place + 1 - 2 * parity, mine)
    has_next, has_previous = place + 2 < sections, place >= 2
    ahead, behind = (place + 2, mine), (place - 2, mine)

    block, depth = x_hbm.shape
    half = block * groups
    tiles, _, tile = weights_in.shape
    per_kind = tiles // 3
    chunks, width, chunk = weights_out.shape
    heads = width // HD
    part = block // PARTS

    def peer(by):
        return (mine + by) % groups

    def source(by):
        return (mine + groups - by) % groups

    def block_at(index):
        return pl.ds(pl.multiple_of(index * block, block), block)

    def remote(src, dst, send, recv, device):
        return pltpu.make_async_remote_copy(
            src_ref=src, dst_ref=dst, send_sem=send, recv_sem=recv, device_id=device, device_id_type=MESH
        )

    def tile_copy(j):
        kind = j // per_kind
        columns = pl.ds(pl.multiple_of((j % per_kind) * tile, tile), tile)
        return pltpu.make_async_copy(weights_in_hbm.at[kind, :, columns], weights_in.at[j], tile_sem.at[j])

    def columns_of(c):
        return pl.ds(pl.multiple_of(c * chunk, chunk), chunk)

    def chunk_copy(c):
        return pltpu.make_async_copy(weights_out_hbm.at[:, columns_of(c)], weights_out.at[c], chunk_sem.at[c])

    def own_rows_copy(c):
        return pltpu.make_async_copy(x_hbm.at[:, columns_of(c)], rows_in.at[0, c], own_row_sem.at[c])

    def fresh_copy(c):
        return pltpu.make_async_copy(
            fresh_hbm.at[parity, :, columns_of(c)], rows_in.at[1, c], next_row_sem.at[c]
        )

    gain_copy = pltpu.make_async_copy(gain_hbm, gain_raw, load_sem.at[0])
    ids_copy = pltpu.make_async_copy(segments_hbm, pieces.at[parity], load_sem.at[1])
    cosine_copy = pltpu.make_async_copy(cosine_hbm, cosine, load_sem.at[2])
    sine_copy = pltpu.make_async_copy(sine_hbm, sine, load_sem.at[3])
    fresh_ids_copy = pltpu.make_async_copy(fresh_segments_hbm, ids.at[1], load_sem.at[4])

    gain_send = remote(gain_pieces.at[parity], gain_pieces.at[parity], small_send.at[0], small_recv.at[0], core)
    ids_send = remote(pieces.at[parity], pieces.at[parity], small_send.at[1], small_recv.at[1], core)
    ids_ahead = remote(ids.at[0], ids.at[1], small_send.at[2], small_recv.at[2], ahead)

    gain_copy.start()
    ids_copy.start()
    for c in range(chunks):
        own_rows_copy(c).start()
    cosine_copy.start()
    sine_copy.start()

    barrier = pltpu.get_barrier_semaphore()
    pl.semaphore_signal(barrier, inc=1, device_id=core, device_id_type=MESH)
    for g in range(1, groups):
        pl.semaphore_signal(barrier, inc=1, device_id=(place, peer(g)), device_id_type=MESH)

    @pl.when(has_next)
    def _():
        pl.semaphore_signal(barrier, inc=1, device_id=ahead, device_id_type=MESH)

    @pl.when(has_previous)
    def _():
        pl.semaphore_signal(barrier, inc=1, device_id=behind, device_id_type=MESH)

    with jax.named_scope("barrier"):
        pl.semaphore_wait(barrier, groups + has_next.astype(jnp.int32) + has_previous.astype(jnp.int32))

    gain_copy.wait()
    gain_pieces[parity] = gain_raw[...].astype(jnp.float32)
    gain_send.start()
    ids_copy.wait()
    ids_send.start()
    for j in range(tiles):
        tile_copy(j).start()
    for c in range(chunks):
        chunk_copy(c).start()

    @pl.when(jnp.logical_not(has_previous))
    def _():
        fresh_ids_copy.start()
        for c in range(chunks):
            fresh_copy(c).start()

    def normalize(step):
        def some(r, carry):
            rows = pl.ds(pl.multiple_of(r * NORM_ROWS, NORM_ROWS), NORM_ROWS)
            power = jnp.zeros((NORM_ROWS, 1), jnp.float32)
            for c in range(chunks):
                widened = rows_in[step, c, rows, :].astype(jnp.float32)
                power = power + jnp.sum(widened * widened, axis=-1, keepdims=True)
            scale = lax.rsqrt(power / depth + eps)
            target = pl.ds(pl.multiple_of(parity * block + r * NORM_ROWS, NORM_ROWS), NORM_ROWS)
            for c in range(chunks):
                columns = slice(c * chunk, (c + 1) * chunk)
                widened = rows_in[step, c, rows, :].astype(jnp.float32)
                gathered[mine, target, columns] = (widened * scale * gain[:, columns]).astype(jnp.bfloat16)
            return carry

        lax.fori_loop(0, block // NORM_ROWS, some, 0)

    def own_copy():
        rows = gathered.at[mine, pl.ds(pl.multiple_of(parity * block, block), block)]
        return remote(rows, rows, own_send.at[0], own_recv.at[0], core)

    def share_copy(g, s):
        rows = gathered.at[mine, pl.ds(pl.multiple_of(parity * block + s * part, part), part)]
        slot = (g - 1) * PARTS + s
        return remote(rows, rows, share_send.at[slot], share_recv.at[slot], (place, peer(g)))

    def relay_copy(g, s, h):
        rows = gathered.at[source(g), pl.ds(h * block + s * part, part)]
        slot = (g - 1) * PARTS + s
        return remote(rows, rows, relay_send.at[slot], relay_recv.at[slot], core)

    def share():
        for s in range(PARTS):
            for g in range(1, groups):
                share_copy(g, s).start()

    def relay(s, h):
        for g in range(1, groups):
            share_copy(g, s).wait_recv()
            relay_copy(g, s, h).start()

    def project(rows, places, first=False, events=(), gate=True):
        def one(j, carry):
            for at, event in events:
                pl.when((j == min(at, tiles - 1)) & gate)(event)
            if first:
                tile_copy(j).wait()
            kind = j // per_kind
            turning = (kind < 2).astype(jnp.float32)
            factor = turning * jnp.where(kind == 0, HD ** (-0.5) * LOG2E, 1.0)
            product = jnp.dot(rows(), weights_in[j], preferred_element_type=jnp.float32)
            column = (j % per_kind) * tile
            for i, token in enumerate(places):
                at = pl.ds(pl.multiple_of(token, block), block)
                cosines = cosine[at, :] * factor + (1.0 - turning)
                sines = sine[at, :] * factor
                for n in range(tile // HD):
                    each = product[i * block : (i + 1) * block, n * HD : (n + 1) * HD]
                    turned = each * cosines + pltpu.roll(each, HD // 2, 1) * sines
                    to = pl.ds(pl.multiple_of(column + n * HD, HD), HD)
                    qkv[kind, at, to] = turned.astype(jnp.bfloat16)
            return carry

        lax.fori_loop(0, tiles, one, 0)

    def project_others(h, events=()):
        def one(g, carry):
            index = source(g)
            project(
                lambda: gathered[index, h * block : (h + 1) * block, :],
                [h * half + index * block],
                events=events,
                gate=g == 1,
            )
            return carry

        lax.fori_loop(1, groups, one, 0)

    def find_bias(step):
        across = half // LANES
        for h in range(2):
            row = jnp.broadcast_to(ids[step, h : h + 1, :].astype(jnp.float32), (LANES, half))
            column = row.T
            for q in range(across):
                wanted = column[q * LANES : (q + 1) * LANES]
                first = h * half + q * LANES
                for k in range(h * across + q + 1):
                    given = ids[step, k // across : k // across + 1, (k % across) * LANES : (k % across + 1) * LANES]
                    seen = wanted == given.astype(jnp.float32)
                    if k == h * across + q:
                        down = lax.broadcasted_iota(jnp.int32, (LANES, LANES), 0)
                        seen = seen & (lax.broadcasted_iota(jnp.int32, (LANES, LANES), 1) <= down)
                    bias[first : first + LANES, k * LANES : (k + 1) * LANES] = jnp.where(seen, 0.0, -1e30)

    def attend(h, low, high):
        def one(n, carry):
            to = pl.ds(pl.multiple_of(n * HD, HD), HD)
            for q in range(half // LANES):
                first = h * half + q * LANES
                last = first + LANES
                scores = lax.dot_general(
                    qkv[0, first:last, to],
                    qkv[1, 0:last, to],
                    (((1,), (1,)), ((), ())),
                    preferred_element_type=jnp.float32,
                ) + bias[first:last, 0:last]
                weights = jnp.exp2(scores - jnp.max(scores, axis=-1, keepdims=True))
                total = jnp.sum(weights, axis=-1, keepdims=True)
                product = jnp.dot(
                    weights.astype(jnp.bfloat16), qkv[2, 0:last, to], preferred_element_type=jnp.float32
                )
                mixed[q * LANES : (q + 1) * LANES, to] = (product / total).astype(jnp.bfloat16)
            return carry

        lax.fori_loop(low, high, one, 0, unroll=min(4, high - low))

    def give_copy(c):
        return remote(partial.at[c], give_in.at[c], give_send.at[c], give_recv.at[c], core)

    def out_products(c):
        for n in range(0, chunk, PIECE):
            columns = slice(n, n + PIECE)
            yield columns, jnp.dot(mixed[...], weights_out[c, :, columns], preferred_element_type=jnp.float32)

    def give(low, high):
        def one(c, carry):
            for columns, product in out_products(c):
                partial[c, :, columns] = product.astype(jnp.bfloat16)
            give_copy(c).start()
            return carry

        lax.fori_loop(low, high, one, 0)

    def wait_given():
        wait_sent([give_copy(c) for c in range(chunks)])

    def multiply():
        def one(c, carry):
            for columns, product in out_products(c):
                partial[c, :, columns] = product.astype(jnp.bfloat16)
            return carry

        lax.fori_loop(0, chunks, one, 0)

    def sum_copy(g, c):
        slot = (g - 1) * chunks + c
        return remote(
            give_in.at[c, block_at(peer(g))], arrived.at[c, g - 1], sum_send.at[slot], sum_recv.at[slot], (place, peer(g))
        )

    def combine(low, high):
        def one(c, carry):
            give_copy(c).wait_recv()
            total = partial[c].astype(jnp.float32) + give_in[c].astype(jnp.float32)
            give_in[c] = total.astype(jnp.bfloat16)
            for g in range(1, groups):
                sum_copy(g, c).start()
            return carry

        lax.fori_loop(low, high, one, 0)

    def store_copy(step, c):
        return pltpu.make_async_copy(staged.at[c], out_hbm.at[step, 0, :, columns_of(c)], store_sem.at[c])

    def shift_copy(c):
        return remote(staged.at[c], rows_in.at[1, c], shift_send.at[c], shift_recv.at[c], ahead)

    def back_copy(c):
        return remote(
            staged.at[c], shadow_hbm.at[0, :, columns_of(c)], back_send.at[c], back_recv.at[c], behind
        )

    def finish(step, low, high):
        def one(c, carry):
            total = rows_in[step, c].astype(jnp.float32) + give_in[c, block_at(mine), :].astype(jnp.float32)
            for g in range(1, groups):
                sum_copy(g, c).wait_recv()
                total = total + arrived[c, g - 1].astype(jnp.float32)
            if step > 0:
                store_copy(0, c).wait()
                pl.when(has_next)(lambda: shift_copy(c).wait_send())
            staged[c] = total.astype(jnp.bfloat16)
            if step == 0:
                pl.when(has_next)(lambda: shift_copy(c).start())
            else:
                pl.when(has_previous)(lambda: back_copy(c).start())
            store_copy(step, c).start()
            return carry

        lax.fori_loop(low, high, one, 0)

    def zero_copy(c):
        return pltpu.make_async_copy(staged.at[0], shadow_hbm.at[0, :, columns_of(c)], back_recv.at[c])

    def wait_sent(copies):
        for copy in copies:
            copy.wait_send()

    every_share = [(g, s) for g in range(1, groups) for s in range(PARTS)]
    is_low, is_high = parity == 0, parity == 1

    scope = jax.named_scope
    ids_send.wait_recv()
    ids[0, 0:1, :] = pieces[0]
    ids[0, 1:2, :] = pieces[1]
    pl.when(has_next)(ids_ahead.start)
    gain_send.wait_recv()
    gain[:, 0 : depth // 2] = gain_pieces[0]
    gain[:, depth // 2 :] = gain_pieces[1]
    for c in range(chunks):
        own_rows_copy(c).wait()
    with scope("norm"):
        normalize(0)
    own_copy().start()
    pl.when(is_low)(share)

    @pl.when(jnp.logical_not(has_next))
    def _():
        staged[0] = jnp.zeros_like(staged[0])
        for c in range(chunks):
            zero_copy(c).start()

    cosine_copy.wait()
    sine_copy.wait()
    with scope("bias"):
        find_bias(0)

    def relay_low(s):
        with scope("early_relay"):
            pl.when(is_low)(lambda: relay(s, 0))

    def combine_low(c):
        with scope("combine"):
            pl.when(is_low)(lambda: combine(c, c + 1))

    def finish_low(step, c):
        with scope("finish"):
            pl.when(is_low)(lambda: finish(step, c, c + 1))

    def free_link():
        @pl.when(is_high)
        def _():
            with scope("finish"):
                finish(0, chunks - 2, chunks - 1)
                wait_sent([sum_copy(g, c) for g in range(1, groups) for c in range(chunks - 1)])
            pl.semaphore_signal(free_sem, inc=1, device_id=core, device_id_type=MESH)

    def share_low():
        @pl.when(is_low)
        def _():
            with scope("wait_free"):
                pl.semaphore_wait(free_sem, 1)
            share()

    def next_rows():
        @pl.when(has_previous)
        def _():
            with scope("wait_shift"):
                ids_ahead.wait_recv()
                for c in range(chunks):
                    shift_copy(c).wait_recv()

        @pl.when(jnp.logical_not(has_previous))
        def _():
            fresh_ids_copy.wait()
            for c in range(chunks):
                fresh_copy(c).wait()

        own_copy().wait_send()
        wait_sent([share_copy(g, s) for g, s in every_share])
        with scope("norm"):
            normalize(1)
        own_copy().start()

    for step in range(2):
        relays = [(at, functools.partial(relay_low, s)) for s, at in enumerate(RELAYS_AT[step])]
        if step == 0:
            with scope("wait_own"):
                own_copy().wait_recv()
            with scope("own"):
                project(lambda: gathered[mine], [mine * block, half + mine * block], True, relays)

            @pl.when(jnp.logical_not(has_next))
            def _():
                for c in range(chunks):
                    zero_copy(c).wait()

            for c in range(chunks):
                chunk_copy(c).wait()
        else:

            @pl.when(is_low)
            def _():
                wait_sent([sum_copy(g, c) for g in range(1, groups) for c in range(chunks)])
                next_rows()

            @pl.when(is_high)
            def _():
                with scope("finish"):
                    finish(0, 0, chunks - 2)
                with scope("wait_own"):
                    own_copy().wait_recv()

            with scope("own_low"):
                project(
                    lambda: gathered[mine, 0:block, :],
                    [mine * block],
                    events=[(FREE_AT, free_link), (SHARE_AT, share_low)],
                )

            @pl.when(is_low)
            def _():
                find_bias(1)
                with scope("wait_own"):
                    own_copy().wait_recv()

            @pl.when(is_high)
            def _():
                with scope("finish"):
                    finish(0, chunks - 1, chunks)
                wait_sent([sum_copy(g, chunks - 1) for g in range(1, groups)])
                next_rows()
                find_bias(1)

            with scope("own_high"):
                project(lambda: gathered[mine, block:, :], [half + mine * block], events=relays)

        @pl.when(is_low)
        def _():
            with scope("late_relay"):
                for s in range(len(RELAYS_AT[step]), PARTS):
                    relay(s, 0)

        @pl.when(is_high)
        def _():
            with scope("wait_relay"):
                for s in range(PARTS):
                    for g in range(1, groups):
                        relay_copy(g, s, 0).wait_recv()
                    if s == PARTS - 2:
                        share()

        with scope("others"):
            project_others(0)
        with scope("attend"):
            attend(0, 0, heads)

        @pl.when(is_low)
        def _():
            wait_sent([relay_copy(g, s, 0) for g, s in every_share])
            if step > 0:
                wait_given()
            with scope("multiply"):
                multiply()
            with scope("combine"):
                combine(0, chunks - len(COMBINES_AT))
            with scope("wait_relay"):
                for g, s in every_share:
                    relay_copy(g, s, 1).wait_recv()

        @pl.when(is_high)
        def _():
            with scope("relay_high"):
                for s in range(PARTS - 1):
                    relay(s, 1)
            with scope("give"):
                give(0, 3)
            with scope("relay_high"):
                relay(PARTS - 1, 1)
            with scope("give"):
                give(3, chunks)

        with scope("others"):
            late = chunks - len(COMBINES_AT)
            events = [(at, functools.partial(combine_low, late + i)) for i, at in enumerate(COMBINES_AT)]
            project_others(1, [*events, (FINISH_AT, functools.partial(finish_low, step, 0))])
        finish_low(step, 1)
        with scope("attend"):
            attend(1, 0, heads // 2)
        finish_low(step, 2)
        with scope("attend"):
            attend(1, heads // 2, heads)

        @pl.when(is_low)
        def _():
            with scope("give"):
                give(0, 2)
        finish_low(step, 3)

        @pl.when(is_low)
        def _():
            with scope("give"):
                give(2, chunks)
            with scope("finish"):
                finish(step, 4, chunks)

        @pl.when(is_high)
        def _():
            wait_sent([relay_copy(g, s, 1) for g, s in every_share])
            wait_given()
            with scope("multiply"):
                multiply()
            with scope("combine"):
                combine(0, chunks)

    @pl.when(is_high)
    def _():
        with scope("finish"):
            finish(1, 0, chunks)

    pl.when(is_low)(wait_given)
    wait_sent([sum_copy(g, c) for g in range(1, groups) for c in range(chunks)])
    own_copy().wait_send()
    wait_sent([share_copy(g, s) for g, s in every_share])
    gain_send.wait_send()
    ids_send.wait_send()
    pl.when(has_next)(ids_ahead.wait_send)
    for c in range(chunks):
        store_copy(1, c).wait()

    @pl.when(has_previous)
    def _():
        wait_sent([back_copy(c) for c in range(chunks)])

    @pl.when(has_next)
    def _():
        with scope("wait_back"):
            for c in range(chunks):
                back_copy(c).wait_recv()


def turning(tokens):
    dim = HD // 2
    frequency = np.float32(rope_base) ** (-(np.arange(dim, dtype=np.float32) * np.float32(2.0 / HD)))
    angles = np.arange(tokens, dtype=np.float32)[:, None] * frequency.astype(np.float32)[None, :]
    cosine, sine = np.cos(angles), np.sin(angles)
    return (
        np.concatenate([cosine, cosine], -1).astype(np.float32),
        np.concatenate([-sine, sine], -1).astype(np.float32),
    )


def per_device(
    groups, sections, carried, carried_segments, fresh_batch, fresh_segments, qkv_weight, out_weight, norm_gain
):
    block, depth = carried.shape[1:]
    half = block * groups
    width = out_weight.shape[1]
    tile = min(TILE, width)
    tiles = 3 * width // tile
    chunks = depth // CHUNK
    cosine, sine = turning(2 * half)
    weights_in = jnp.transpose(qkv_weight[0], (1, 0, 2))
    near, f32 = jnp.bfloat16, jnp.float32
    dma = pltpu.SemaphoreType.DMA
    shares = (groups - 1) * PARTS
    sums = (groups - 1) * chunks
    flops = 2 * (2 * 2 * half * depth * 4 * width + 4 * width * 4 * half * half)
    out, shadow = pl.pallas_call(
        functools.partial(relay_kernel, groups, sections),
        out_shape=(
            jax.ShapeDtypeStruct((2, 1, block, depth), near),
            jax.ShapeDtypeStruct((1, block, depth), near),
        ),
        in_specs=[pl.BlockSpec(memory_space=pl.ANY)] * 9,
        out_specs=(pl.BlockSpec(memory_space=pl.ANY),) * 2,
        scratch_shapes=[
            pltpu.VMEM((tiles, depth, tile), near),
            pltpu.VMEM((chunks, width, CHUNK), near),
            pltpu.VMEM((groups, 2 * block, depth), near),
            pltpu.VMEM((3, 2 * half, width), near),
            pltpu.VMEM((half, width), near),
            pltpu.VMEM((chunks, half, CHUNK), near),
            pltpu.VMEM((chunks, half, CHUNK), near),
            pltpu.VMEM((chunks, groups - 1, block, CHUNK), near),
            pltpu.VMEM((2, chunks, block, CHUNK), near),
            pltpu.VMEM((chunks, block, CHUNK), near),
            pltpu.VMEM((2 * half, HD), f32),
            pltpu.VMEM((2 * half, HD), f32),
            pltpu.VMEM((2 * half, 2 * half), f32),
            pltpu.VMEM((2, 1, half), jnp.int32),
            pltpu.VMEM((2, 2, half), jnp.int32),
            pltpu.VMEM((1, depth // 2), near),
            pltpu.VMEM((2, 1, depth // 2), f32),
            pltpu.VMEM((1, depth), f32),
            dma((5,)),
            dma((tiles,)),
            dma((chunks,)),
            dma((chunks,)),
            dma((chunks,)),
            dma((3,)),
            dma((3,)),
            dma((1,)),
            dma((1,)),
            dma((shares,)),
            dma((shares,)),
            dma((shares,)),
            dma((shares,)),
            dma((chunks,)),
            dma((chunks,)),
            dma((sums,)),
            dma((sums,)),
            dma((chunks,)),
            dma((chunks,)),
            dma((chunks,)),
            dma((chunks,)),
            dma((chunks,)),
            pltpu.SemaphoreType.REGULAR,
        ],
        compiler_params=pltpu.CompilerParams(
            collective_id=0, has_side_effects=True, vmem_limit_bytes=67043328
        ),
        cost_estimate=pl.CostEstimate(
            flops=flops, bytes_accessed=8 * depth * width, transcendentals=0
        ),
        name="relay",
    )(
        carried[0],
        carried_segments,
        fresh_batch,
        fresh_segments,
        weights_in,
        out_weight[0],
        norm_gain,
        cosine,
        sine,
    )
    return out, shadow


def solution(mesh):
    return jax.shard_map(
        functools.partial(per_device, mesh.shape["tp"], mesh.shape["section"]),
        mesh=mesh,
        in_specs=(
            P("section", "tp", None),
            P("section", None),
            P(None, "tp", None),
            P(),
            P("section", None, None, "tp"),
            P("section", "tp", None),
            P("section", None),
        ),
        out_specs=(P(None, "section", "tp", None), P("section", "tp", None)),
        check_vma=False,
    )
```

```python
import functools

import jax
import jax.numpy as jnp
import numpy as np
from jax import lax
from jax.experimental import pallas as pl
from jax.experimental.pallas import tpu as pltpu
from jax.sharding import PartitionSpec as P

HD = 128
LANES = 128
LOG2E = 1.4426950408889634
TILE = 512
CHUNK = 1024
UNIT = 1
PARTS = 4
NORM_ROWS = 16
PIECE = 256
PIECES = 4
RELAYS_AT = ((3, 5), (0, 0, 3, 5))
COMBINES_AT = (1, 2, 3)
FREE_AT = 3
LAST_AT = 5
SHARE_AT = 4
FINISH_AT = 4
MESH = pl.DeviceIdType.MESH

eps = 1e-05
rope_base = 10000.0


def relay_kernel(
    groups,
    sections,
    x_hbm,
    segments_hbm,
    fresh_hbm,
    fresh_segments_hbm,
    weights_in_hbm,
    weights_out_hbm,
    gain_hbm,
    cosine_hbm,
    sine_hbm,
    first_hbm,
    second_hbm,
    shadow_hbm,
    weights_in,
    weights_out,
    gathered,
    qkv,
    mixed,
    partial,
    give_in,
    arrived,
    rows_in,
    staged,
    cosine,
    sine,
    bias,
    pieces,
    ids,
    gain_raw,
    gain_pieces,
    gain,
    load_sem,
    tile_sem,
    chunk_sem,
    own_row_sem,
    next_row_sem,
    small_send,
    small_recv,
    own_send,
    own_recv,
    share_send,
    share_recv,
    relay_send,
    relay_recv,
    give_send,
    give_recv,
    sum_send,
    sum_recv,
    shift_send,
    shift_recv,
    back_send,
    back_recv,
    store_sem,
    free_sem,
):
    place = lax.axis_index("section")
    mine = lax.axis_index("tp")
    parity = place % 2
    core = (place + 1 - 2 * parity, mine)
    has_next, has_previous = place + 2 < sections, place >= 2
    ahead, behind = (place + 2, mine), (place - 2, mine)

    block, depth = x_hbm.shape
    half = block * groups
    tiles, _, tile = weights_in.shape
    per_kind = tiles // 3
    chunks, width, chunk = weights_out.shape
    heads = width // HD
    part = block // PARTS

    def peer(by):
        return (mine + by) % groups

    def source(by):
        return (mine + groups - by) % groups

    def block_at(index):
        return pl.ds(pl.multiple_of(index * block, block), block)

    def remote(src, dst, send, recv, device):
        return pltpu.make_async_remote_copy(
            src_ref=src, dst_ref=dst, send_sem=send, recv_sem=recv, device_id=device, device_id_type=MESH
        )

    def tile_copy(j):
        kind = j // per_kind
        columns = pl.ds(pl.multiple_of((j % per_kind) * tile, tile), tile)
        return pltpu.make_async_copy(weights_in_hbm.at[kind, :, columns], weights_in.at[j], tile_sem.at[j])

    def columns_of(c):
        return pl.ds(pl.multiple_of(c * chunk, chunk), chunk)

    def chunk_copy(c):
        return pltpu.make_async_copy(weights_out_hbm.at[:, columns_of(c)], weights_out.at[c], chunk_sem.at[c])

    def own_rows_copy(c):
        return pltpu.make_async_copy(x_hbm.at[:, columns_of(c)], rows_in.at[0, c], own_row_sem.at[c])

    def fresh_copy(c):
        return pltpu.make_async_copy(
            fresh_hbm.at[parity, :, columns_of(c)], rows_in.at[1, c], next_row_sem.at[c]
        )

    gain_copy = pltpu.make_async_copy(gain_hbm, gain_raw, load_sem.at[0])
    ids_copy = pltpu.make_async_copy(segments_hbm, pieces.at[parity], load_sem.at[1])
    cosine_copy = pltpu.make_async_copy(cosine_hbm, cosine, load_sem.at[2])
    sine_copy = pltpu.make_async_copy(sine_hbm, sine, load_sem.at[3])
    fresh_ids_copy = pltpu.make_async_copy(fresh_segments_hbm, ids.at[1], load_sem.at[4])

    gain_send = remote(gain_pieces.at[parity], gain_pieces.at[parity], small_send.at[0], small_recv.at[0], core)
    ids_send = remote(pieces.at[parity], pieces.at[parity], small_send.at[1], small_recv.at[1], core)
    ids_ahead = remote(ids.at[0], ids.at[1], small_send.at[2], small_recv.at[2], ahead)

    gain_copy.start()
    ids_copy.start()
    for c in range(chunks):
        own_rows_copy(c).start()
    cosine_copy.start()
    sine_copy.start()

    barrier = pltpu.get_barrier_semaphore()
    pl.semaphore_signal(barrier, inc=1, device_id=core, device_id_type=MESH)
    for g in range(1, groups):
        pl.semaphore_signal(barrier, inc=1, device_id=(place, peer(g)), device_id_type=MESH)

    @pl.when(has_next)
    def _():
        pl.semaphore_signal(barrier, inc=1, device_id=ahead, device_id_type=MESH)

    @pl.when(has_previous)
    def _():
        pl.semaphore_signal(barrier, inc=1, device_id=behind, device_id_type=MESH)

    with jax.named_scope("barrier"):
        pl.semaphore_wait(barrier, groups + has_next.astype(jnp.int32) + has_previous.astype(jnp.int32))

    gain_copy.wait()
    gain_pieces[parity] = gain_raw[...].astype(jnp.float32)
    gain_send.start()
    ids_copy.wait()
    ids_send.start()
    for j in range(tiles):
        tile_copy(j).start()
    for c in range(chunks):
        chunk_copy(c).start()

    @pl.when(jnp.logical_not(has_previous))
    def _():
        fresh_ids_copy.start()
        for c in range(chunks):
            fresh_copy(c).start()

    def normalize(step):
        def some(r, carry):
            rows = pl.ds(pl.multiple_of(r * NORM_ROWS, NORM_ROWS), NORM_ROWS)
            power = jnp.zeros((NORM_ROWS, 1), jnp.float32)
            for c in range(chunks):
                widened = rows_in[step, c, rows, :].astype(jnp.float32)
                power = power + jnp.sum(widened * widened, axis=-1, keepdims=True)
            scale = lax.rsqrt(power / depth + eps)
            target = pl.ds(pl.multiple_of(parity * block + r * NORM_ROWS, NORM_ROWS), NORM_ROWS)
            for c in range(chunks):
                columns = slice(c * chunk, (c + 1) * chunk)
                widened = rows_in[step, c, rows, :].astype(jnp.float32)
                gathered[mine, target, columns] = (widened * scale * gain[:, columns]).astype(jnp.bfloat16)
            return carry

        lax.fori_loop(0, block // NORM_ROWS, some, 0)

    def own_copy():
        rows = gathered.at[mine, pl.ds(pl.multiple_of(parity * block, block), block)]
        return remote(rows, rows, own_send.at[0], own_recv.at[0], core)

    def share_copy(g, s):
        rows = gathered.at[mine, pl.ds(pl.multiple_of(parity * block + s * part, part), part)]
        slot = (g - 1) * PARTS + s
        return remote(rows, rows, share_send.at[slot], share_recv.at[slot], (place, peer(g)))

    def relay_copy(g, s, h):
        rows = gathered.at[source(g), pl.ds(h * block + s * part, part)]
        slot = (g - 1) * PARTS + s
        return remote(rows, rows, relay_send.at[slot], relay_recv.at[slot], core)

    def share():
        for s in range(PARTS):
            for g in range(1, groups):
                share_copy(g, s).start()

    def relay(s, h):
        for g in range(1, groups):
            share_copy(g, s).wait_recv()
            relay_copy(g, s, h).start()

    def project(rows, places, first=False, events=(), gate=True):
        def one(j, carry):
            for at, event in events:
                pl.when((j == min(at, tiles - 1)) & gate)(event)
            if first:
                tile_copy(j).wait()
            kind = j // per_kind
            turning = (kind < 2).astype(jnp.float32)
            factor = turning * jnp.where(kind == 0, HD ** (-0.5) * LOG2E, 1.0)
            product = jnp.dot(rows(), weights_in[j], preferred_element_type=jnp.float32)
            column = (j % per_kind) * tile
            for i, token in enumerate(places):
                at = pl.ds(pl.multiple_of(token, block), block)
                cosines = cosine[at, :] * factor + (1.0 - turning)
                sines = sine[at, :] * factor
                for n in range(tile // HD):
                    each = product[i * block : (i + 1) * block, n * HD : (n + 1) * HD]
                    turned = each * cosines + pltpu.roll(each, HD // 2, 1) * sines
                    to = pl.ds(pl.multiple_of(column + n * HD, HD), HD)
                    qkv[kind, at, to] = turned.astype(jnp.bfloat16)
            return carry

        lax.fori_loop(0, tiles, one, 0)

    def project_others(h, events=()):
        def one(g, carry):
            index = source(g)
            project(
                lambda: gathered[index, h * block : (h + 1) * block, :],
                [h * half + index * block],
                events=events,
                gate=g == 1,
            )
            return carry

        lax.fori_loop(1, groups, one, 0)

    def find_bias(step):
        across = half // LANES
        for h in range(2):
            row = jnp.broadcast_to(ids[step, h : h + 1, :].astype(jnp.float32), (LANES, half))
            column = row.T
            for q in range(across):
                wanted = column[q * LANES : (q + 1) * LANES]
                first = h * half + q * LANES
                for k in range(h * across + q + 1):
                    given = ids[step, k // across : k // across + 1, (k % across) * LANES : (k % across + 1) * LANES]
                    seen = wanted == given.astype(jnp.float32)
                    if k == h * across + q:
                        down = lax.broadcasted_iota(jnp.int32, (LANES, LANES), 0)
                        seen = seen & (lax.broadcasted_iota(jnp.int32, (LANES, LANES), 1) <= down)
                    bias[first : first + LANES, k * LANES : (k + 1) * LANES] = jnp.where(seen, 0.0, -1e30)

    def attend(h, low, high):
        def one(n, carry):
            to = pl.ds(pl.multiple_of(n * HD, HD), HD)
            for q in range(half // LANES):
                first = h * half + q * LANES
                last = first + LANES
                scores = lax.dot_general(
                    qkv[0, first:last, to],
                    qkv[1, 0:last, to],
                    (((1,), (1,)), ((), ())),
                    preferred_element_type=jnp.float32,
                ) + bias[first:last, 0:last]
                weights = jnp.exp2(scores - jnp.max(scores, axis=-1, keepdims=True))
                total = jnp.sum(weights, axis=-1, keepdims=True)
                product = jnp.dot(
                    weights.astype(jnp.bfloat16), qkv[2, 0:last, to], preferred_element_type=jnp.float32
                )
                mixed[q * LANES : (q + 1) * LANES, to] = (product / total).astype(jnp.bfloat16)
            return carry

        lax.fori_loop(low, high, one, 0, unroll=min(4, high - low))

    def give_copy(c):
        return remote(partial.at[c], give_in.at[c], give_send.at[c], give_recv.at[c], core)

    def out_products(c):
        for n in range(0, chunk, PIECE):
            columns = slice(n, n + PIECE)
            yield columns, jnp.dot(mixed[...], weights_out[c, :, columns], preferred_element_type=jnp.float32)

    def give(low, high):
        def one(c, carry):
            for columns, product in out_products(c):
                partial[c, :, columns] = product.astype(jnp.bfloat16)
            give_copy(c).start()
            return carry

        lax.fori_loop(low, high, one, 0)

    def wait_given():
        wait_sent([give_copy(c) for c in range(chunks)])

    def multiply():
        def one(c, carry):
            for columns, product in out_products(c):
                partial[c, :, columns] = product.astype(jnp.bfloat16)
            return carry

        lax.fori_loop(0, chunks, one, 0)

    def sum_copy(g, c):
        slot = (g - 1) * chunks + c
        return remote(
            give_in.at[c, block_at(peer(g))], arrived.at[c, g - 1], sum_send.at[slot], sum_recv.at[slot], (place, peer(g))
        )

    def combine(low, high):
        def one(c, carry):
            give_copy(c).wait_recv()
            total = partial[c].astype(jnp.float32) + give_in[c].astype(jnp.float32)
            give_in[c] = total.astype(jnp.bfloat16)
            for g in range(1, groups):
                sum_copy(g, c).start()
            return carry

        lax.fori_loop(low, high, one, 0)

    def store_copy(step, c):
        out = second_hbm if step else first_hbm
        return pltpu.make_async_copy(staged.at[c], out.at[:, columns_of(c)], store_sem.at[c])

    def shift_copy(c):
        return remote(staged.at[c], rows_in.at[1, c], shift_send.at[c], shift_recv.at[c], ahead)

    def back_copy(c):
        return remote(
            staged.at[c], shadow_hbm.at[0, :, columns_of(c)], back_send.at[c], back_recv.at[c], behind
        )

    def finish(step, low, high):
        def one(c, carry):
            total = rows_in[step, c].astype(jnp.float32) + give_in[c, block_at(mine), :].astype(jnp.float32)
            for g in range(1, groups):
                sum_copy(g, c).wait_recv()
                total = total + arrived[c, g - 1].astype(jnp.float32)
            if step > 0:
                store_copy(0, c).wait()
                pl.when(has_next)(lambda: shift_copy(c).wait_send())
            staged[c] = total.astype(jnp.bfloat16)
            if step == 0:
                pl.when(has_next)(lambda: shift_copy(c).start())
            else:
                pl.when(has_previous)(lambda: back_copy(c).start())
            store_copy(step, c).start()
            return carry

        lax.fori_loop(low, high, one, 0)

    def zero_copy(c):
        return pltpu.make_async_copy(staged.at[0], shadow_hbm.at[0, :, columns_of(c)], back_recv.at[c])

    def wait_sent(copies):
        for copy in copies:
            copy.wait_send()

    every_share = [(g, s) for g in range(1, groups) for s in range(PARTS)]
    is_low, is_high = parity == 0, parity == 1

    scope = jax.named_scope
    ids_send.wait_recv()
    ids[0, 0:1, :] = pieces[0]
    ids[0, 1:2, :] = pieces[1]
    pl.when(has_next)(ids_ahead.start)
    gain_send.wait_recv()
    gain[:, 0 : depth // 2] = gain_pieces[0]
    gain[:, depth // 2 :] = gain_pieces[1]
    for c in range(chunks):
        own_rows_copy(c).wait()
    with scope("norm"):
        normalize(0)
    own_copy().start()
    pl.when(is_low)(share)

    @pl.when(jnp.logical_not(has_next))
    def _():
        staged[0] = jnp.zeros_like(staged[0])
        for c in range(chunks):
            zero_copy(c).start()

    cosine_copy.wait()
    sine_copy.wait()
    with scope("bias"):
        find_bias(0)

    def relay_low(s):
        with scope("early_relay"):
            pl.when(is_low)(lambda: relay(s, 0))

    def combine_low(u):
        with scope("combine"):
            pl.when(is_low)(lambda: combine(u * UNIT, (u + 1) * UNIT))

    def finish_low(step, u):
        with scope("finish"):
            pl.when(is_low)(lambda: finish(step, u * UNIT, (u + 1) * UNIT))

    def finish_last():
        with scope("finish"):
            pl.when(is_high)(lambda: finish(0, chunks - 1, chunks))

    def free_link():
        @pl.when(is_high)
        def _():
            with scope("finish"):
                finish(0, chunks - 2, chunks - 1)
                wait_sent([sum_copy(g, c) for g in range(1, groups) for c in range(chunks - 1)])
            pl.semaphore_signal(free_sem, inc=1, device_id=core, device_id_type=MESH)

    def share_low():
        @pl.when(is_low)
        def _():
            with scope("wait_free"):
                pl.semaphore_wait(free_sem, 1)
            share()

    def next_rows():
        @pl.when(has_previous)
        def _():
            with scope("wait_shift"):
                ids_ahead.wait_recv()
                for c in range(chunks):
                    shift_copy(c).wait_recv()

        @pl.when(jnp.logical_not(has_previous))
        def _():
            fresh_ids_copy.wait()
            for c in range(chunks):
                fresh_copy(c).wait()

        own_copy().wait_send()
        wait_sent([share_copy(g, s) for g, s in every_share])
        with scope("norm"):
            normalize(1)
        own_copy().start()

    for step in range(2):
        relays = [(at, functools.partial(relay_low, s)) for s, at in enumerate(RELAYS_AT[step])]
        if step == 0:
            with scope("wait_own"):
                own_copy().wait_recv()
            with scope("own"):
                project(lambda: gathered[mine], [mine * block, half + mine * block], True, relays)

            @pl.when(jnp.logical_not(has_next))
            def _():
                for c in range(chunks):
                    zero_copy(c).wait()

            for c in range(chunks):
                chunk_copy(c).wait()
        else:

            @pl.when(is_low)
            def _():
                wait_sent([sum_copy(g, c) for g in range(1, groups) for c in range(chunks)])
                next_rows()

            @pl.when(is_high)
            def _():
                with scope("finish"):
                    finish(0, 0, chunks - 2)
                with scope("wait_own"):
                    own_copy().wait_recv()

            with scope("own_low"):
                project(
                    lambda: gathered[mine, 0:block, :],
                    [mine * block],
                    events=[(FREE_AT, free_link), (LAST_AT, finish_last), (SHARE_AT, share_low)],
                )

            @pl.when(is_low)
            def _():
                find_bias(1)
                with scope("wait_own"):
                    own_copy().wait_recv()

            @pl.when(is_high)
            def _():
                wait_sent([sum_copy(g, chunks - 1) for g in range(1, groups)])
                next_rows()
                find_bias(1)

            with scope("own_high"):
                project(lambda: gathered[mine, block:, :], [half + mine * block], events=relays)

        @pl.when(is_low)
        def _():
            with scope("late_relay"):
                for s in range(len(RELAYS_AT[step]), PARTS):
                    relay(s, 0)

        @pl.when(is_high)
        def _():
            with scope("wait_relay"):
                for s in range(PARTS):
                    for g in range(1, groups):
                        relay_copy(g, s, 0).wait_recv()
                    if s == PARTS - 2:
                        share()

        with scope("others"):
            project_others(0)
        with scope("attend"):
            attend(0, 0, heads)

        @pl.when(is_low)
        def _():
            wait_sent([relay_copy(g, s, 0) for g, s in every_share])
            if step > 0:
                wait_given()
            with scope("multiply"):
                multiply()
            with scope("combine"):
                combine(0, chunks - UNIT * len(COMBINES_AT))
            with scope("wait_relay"):
                for g, s in every_share:
                    relay_copy(g, s, 1).wait_recv()

        @pl.when(is_high)
        def _():
            with scope("relay_high"):
                for s in range(PARTS - 1):
                    relay(s, 1)
            with scope("give"):
                give(0, 3 * UNIT)
            with scope("relay_high"):
                relay(PARTS - 1, 1)
            with scope("give"):
                give(3 * UNIT, chunks)

        with scope("others"):
            late = chunks // UNIT - len(COMBINES_AT)
            events = [(at, functools.partial(combine_low, late + i)) for i, at in enumerate(COMBINES_AT)]
            project_others(1, [*events, (FINISH_AT, functools.partial(finish_low, step, 0))])
        finish_low(step, 1)
        with scope("attend"):
            attend(1, 0, heads // 2)
        finish_low(step, 2)
        with scope("attend"):
            attend(1, heads // 2, heads)

        @pl.when(is_low)
        def _():
            with scope("give"):
                give(0, 2 * UNIT)
        finish_low(step, 3)

        @pl.when(is_low)
        def _():
            with scope("give"):
                give(2 * UNIT, chunks)
            with scope("finish"):
                finish(step, 4 * UNIT, chunks)

        @pl.when(is_high)
        def _():
            wait_sent([relay_copy(g, s, 1) for g, s in every_share])
            wait_given()
            with scope("multiply"):
                multiply()
            with scope("combine"):
                combine(0, chunks)

    @pl.when(is_high)
    def _():
        with scope("finish"):
            finish(1, 0, chunks)

    pl.when(is_low)(wait_given)
    wait_sent([sum_copy(g, c) for g in range(1, groups) for c in range(chunks)])
    own_copy().wait_send()
    wait_sent([share_copy(g, s) for g, s in every_share])
    gain_send.wait_send()
    ids_send.wait_send()
    pl.when(has_next)(ids_ahead.wait_send)
    for c in range(chunks):
        store_copy(1, c).wait()

    @pl.when(has_previous)
    def _():
        wait_sent([back_copy(c) for c in range(chunks)])

    @pl.when(has_next)
    def _():
        with scope("wait_back"):
            for c in range(chunks):
                back_copy(c).wait_recv()


def collect_kernel(first, second, shadow, out, back, held, load_sem, store_sem):
    rows = first.shape[0] // PIECES
    moves = []
    for source, target in ((first, out.at[0, 0]), (second, out.at[1, 0]), (shadow.at[0], back.at[0])):
        for n in range(PIECES):
            part, slot = pl.ds(n * rows, rows), len(moves)
            load = pltpu.make_async_copy(source.at[part], held.at[slot], load_sem.at[slot])
            store = pltpu.make_async_copy(held.at[slot], target.at[part], store_sem.at[slot])
            load.start()
            moves.append((load, store))
    for load, store in moves:
        load.wait()
        store.start()
    for _, store in moves:
        store.wait()


def collect(first, second, shadow):
    block, depth = first.shape
    near, count = first.dtype, 3 * PIECES
    return pl.pallas_call(
        collect_kernel,
        out_shape=(
            jax.ShapeDtypeStruct((2, 1, block, depth), near),
            jax.ShapeDtypeStruct((1, block, depth), near),
        ),
        in_specs=[pl.BlockSpec(memory_space=pl.ANY)] * 3,
        out_specs=(pl.BlockSpec(memory_space=pl.ANY),) * 2,
        scratch_shapes=[
            pltpu.VMEM((count, block // PIECES, depth), near),
            pltpu.SemaphoreType.DMA((count,)),
            pltpu.SemaphoreType.DMA((count,)),
        ],
        compiler_params=pltpu.CompilerParams(vmem_limit_bytes=67043328),
        name="collect",
    )(first, second, shadow)


def turning(tokens):
    dim = HD // 2
    frequency = np.float32(rope_base) ** (-(np.arange(dim, dtype=np.float32) * np.float32(2.0 / HD)))
    angles = np.arange(tokens, dtype=np.float32)[:, None] * frequency.astype(np.float32)[None, :]
    cosine, sine = np.cos(angles), np.sin(angles)
    return (
        np.concatenate([cosine, cosine], -1).astype(np.float32),
        np.concatenate([-sine, sine], -1).astype(np.float32),
    )


def per_device(
    groups, sections, carried, carried_segments, fresh_batch, fresh_segments, qkv_weight, out_weight, norm_gain
):
    block, depth = carried.shape[1:]
    half = block * groups
    width = out_weight.shape[1]
    tile = min(TILE, width)
    tiles = 3 * width // tile
    chunks = depth // CHUNK
    cosine, sine = turning(2 * half)
    weights_in = jnp.transpose(qkv_weight[0], (1, 0, 2))
    near, f32 = jnp.bfloat16, jnp.float32
    dma = pltpu.SemaphoreType.DMA
    shares = (groups - 1) * PARTS
    sums = (groups - 1) * chunks
    flops = 2 * (2 * 2 * half * depth * 4 * width + 4 * width * 4 * half * half)
    first, second, shadow = pl.pallas_call(
        functools.partial(relay_kernel, groups, sections),
        out_shape=(
            jax.ShapeDtypeStruct((block, depth), near),
            jax.ShapeDtypeStruct((block, depth), near),
            jax.ShapeDtypeStruct((1, block, depth), near),
        ),
        in_specs=[pl.BlockSpec(memory_space=pl.ANY)] * 9,
        out_specs=(pl.BlockSpec(memory_space=pl.ANY),) * 3,
        scratch_shapes=[
            pltpu.VMEM((tiles, depth, tile), near),
            pltpu.VMEM((chunks, width, CHUNK), near),
            pltpu.VMEM((groups, 2 * block, depth), near),
            pltpu.VMEM((3, 2 * half, width), near),
            pltpu.VMEM((half, width), near),
            pltpu.VMEM((chunks, half, CHUNK), near),
            pltpu.VMEM((chunks, half, CHUNK), near),
            pltpu.VMEM((chunks, groups - 1, block, CHUNK), near),
            pltpu.VMEM((2, chunks, block, CHUNK), near),
            pltpu.VMEM((chunks, block, CHUNK), near),
            pltpu.VMEM((2 * half, HD), f32),
            pltpu.VMEM((2 * half, HD), f32),
            pltpu.VMEM((2 * half, 2 * half), f32),
            pltpu.VMEM((2, 1, half), jnp.int32),
            pltpu.VMEM((2, 2, half), jnp.int32),
            pltpu.VMEM((1, depth // 2), near),
            pltpu.VMEM((2, 1, depth // 2), f32),
            pltpu.VMEM((1, depth), f32),
            dma((5,)),
            dma((tiles,)),
            dma((chunks,)),
            dma((chunks,)),
            dma((chunks,)),
            dma((3,)),
            dma((3,)),
            dma((1,)),
            dma((1,)),
            dma((shares,)),
            dma((shares,)),
            dma((shares,)),
            dma((shares,)),
            dma((chunks,)),
            dma((chunks,)),
            dma((sums,)),
            dma((sums,)),
            dma((chunks,)),
            dma((chunks,)),
            dma((chunks,)),
            dma((chunks,)),
            dma((chunks,)),
            pltpu.SemaphoreType.REGULAR,
        ],
        compiler_params=pltpu.CompilerParams(
            collective_id=0, has_side_effects=True, vmem_limit_bytes=67043328
        ),
        cost_estimate=pl.CostEstimate(
            flops=flops, bytes_accessed=8 * depth * width, transcendentals=0
        ),
        name="relay",
    )(
        carried[0],
        carried_segments,
        fresh_batch,
        fresh_segments,
        weights_in,
        out_weight[0],
        norm_gain,
        cosine,
        sine,
    )
    return collect(first, second, shadow)


def solution(mesh):
    return jax.shard_map(
        functools.partial(per_device, mesh.shape["tp"], mesh.shape["section"]),
        mesh=mesh,
        in_specs=(
            P("section", "tp", None),
            P("section", None),
            P(None, "tp", None),
            P(),
            P("section", None, None, "tp"),
            P("section", "tp", None),
            P("section", None),
        ),
        out_specs=(P(None, "section", "tp", None), P("section", "tp", None)),
        check_vma=False,
    )
```
